256 devices in a mesh: groups: 2 (over y), seq: 128 (over z, x, core).
Axes of the slice: x: 4, y: 2, z: 16, core: 2. Of those that a mesh axis runs over, the one named last changes fastest.
The devices are a block of a 4x16x16 slice.
Arguments:
- queries: bfloat16 [65536, 2048], P(('groups', 'seq')), parts along dimension 0, may hold values from -20 to 20
- keys: bfloat16 [65536, 2048], P(('groups', 'seq')), parts along dimension 0, may hold values from -20 to 20
- values: bfloat16 [65536, 2048], P(('groups', 'seq')), parts along dimension 0, may hold values from -6 to 6
- block_counts: int32 [128], P('groups'), parts along dimension 0, may hold values from 2 to 6, as said below
- last_tokens: int32 [256], P('groups'), parts along dimension 0, may hold values from 64 to 128
- pack_order: int32 [256], P('groups'), parts along dimension 0, may hold values from 0 to 127, as said below
- decode_slot: int32 [128], P('groups'), parts along dimension 0, may hold values from 0 to 63, each once
Outputs:
- attended: bfloat16 [65536, 2048], P(('groups', 'seq')), parts along dimension 0
- cache_keys: bfloat16 [256, 256, 16, 128], P(('groups', 'seq')), parts along dimension 0
- cache_values: bfloat16 [256, 256, 16, 128], P(('groups', 'seq')), parts along dimension 0
The draws below stay inside these ranges and needn't reach their ends.
There are 2 independent parts, one for each index of `groups`. The reference program is written for one: setup_inputs(seed, part) draws one part's arguments, and reference() takes and returns one part's arrays. A program takes and returns all parts, laid end to end along the dimension named above; each array names one. Nothing has to cross between parts.
Inputs may be any that keep to these rules, and one draw needn't show every extreme that they name: `block_counts`: they sum to 192; the largest equals 6. `pack_order`: each prompt number appears once. The last 1 positions hold null prompts, and the position before them a conditional prompt of 6 blocks. `decode_slot`: each slot appears once.
All inputs are finite; a program needn't handle non-finite values.
Results may differ from the reference program's by a relative error of at most 0.0034.
Values may be sent and summed in bfloat16 or wider, within the bound.
A program may use at most 64 MiB of HBM per device.

```python
import jax
import jax.numpy as jnp
from jax import lax

HEADS = 16
HEAD_DIM = 128
BLOCK = 128
MAXB = 6
BLK_DEV = 2
NB = 256
TOKENS = 32768
PAIRS = 64
SPLITS = 8
SLICE = 16


def draw_queries(key, part):
    noise = jnp.clip(jax.random.normal(jax.random.fold_in(key, 1), (TOKENS, HEADS * HEAD_DIM), jnp.float32), -6.0, 6.0)
    return noise.astype(jnp.bfloat16)


def draw_keys(key, part):
    noise = jnp.clip(jax.random.normal(jax.random.fold_in(key, 2), (TOKENS, HEADS * HEAD_DIM), jnp.float32), -6.0, 6.0)
    return noise.astype(jnp.bfloat16)


def pack_plan(key):
    base = jax.random.fold_in(key, 11)
    first_key, second_key, third_key, fourth_key = jax.random.split(base, 4)
    pair_ids = jnp.arange(PAIRS, dtype=jnp.int32)
    biggest = jax.random.randint(first_key, (), 0, PAIRS).astype(jnp.int32)
    counts = jnp.where(pair_ids == biggest, MAXB, 2).astype(jnp.int32)
    extra = NB - PAIRS - (2 * (PAIRS - 1) + MAXB)

    def add_one(step, current):
        scores = jax.random.randint(jax.random.fold_in(second_key, step), (PAIRS,), 0, 1 << 20).astype(jnp.int32) * PAIRS + pair_ids
        scores = jnp.where(current < MAXB, scores, -1)
        chosen = jnp.argmax(scores).astype(jnp.int32)
        return current + (pair_ids == chosen).astype(jnp.int32)
    counts = lax.fori_loop(0, extra, add_one, counts)
    null_order = jax.random.permutation(third_key, PAIRS).astype(jnp.int32)
    tail_nulls = PAIRS + null_order[:BLK_DEV - 1]
    spare_nulls = PAIRS + null_order[BLK_DEV - 1:]
    spare_count = PAIRS - BLK_DEV + 1
    cond_order = jax.random.permutation(fourth_key, PAIRS).astype(jnp.int32)
    rank_keys = jnp.where(cond_order == biggest, PAIRS, pair_ids).astype(jnp.int32)
    cond_seq = cond_order[jnp.argsort(rank_keys, stable=True)][:PAIRS - 1]
    first_edge = BLK_DEV
    middle_edge = NB // BLK_DEV // 2 * BLK_DEV
    order = jnp.zeros((2 * PAIRS,), jnp.int32)

    def place(step, carry):
        current, write, start, queue = carry
        prompt = cond_seq[step]
        size = counts[prompt]
        filler = (start + size == first_edge) | (start + size == middle_edge)
        current = current.at[write].set(jnp.where(filler, spare_nulls[queue], prompt))
        bump = filler.astype(jnp.int32)
        write = write + bump
        start = start + bump
        queue = queue + bump
        current = current.at[write].set(prompt)
        return (current, write + 1, start + size, queue)
    zero = jnp.zeros((), jnp.int32)
    order, write, start, queue = lax.fori_loop(0, PAIRS - 1, place, (order, zero, zero, zero))

    def rest(index, current):
        keep = index >= queue
        target = jnp.where(keep, write + index - queue, 2 * PAIRS - 1).astype(jnp.int32)
        return current.at[target].set(jnp.where(keep, spare_nulls[index], current[target]))
    order = lax.fori_loop(0, spare_count, rest, order)
    order = order.at[2 * PAIRS - BLK_DEV].set(biggest)
    order = order.at[2 * PAIRS - BLK_DEV + 1:].set(tail_nulls)
    return (counts, order.astype(jnp.int32))


def draw_block_counts(key, part):
    counts, order = pack_plan(key)
    return counts


def draw_pack_order(key, part):
    counts, order = pack_plan(key)
    return order


def touch_ends(array, rng, smallest, high):
    shape = array.shape
    spot = [jax.random.randint(jax.random.fold_in(rng, axis), (), 0, shape[axis]) for axis in range(len(shape))]
    array = array.at[tuple(spot)].set(smallest)
    longest = shape.index(max(shape))
    spot[longest] = (spot[longest] + 1) % shape[longest]
    return array.at[tuple(spot)].set(high)


def levels(rng, shape, cuts, smallest, largest):
    factor_of = 1.0
    for dim, parts in cuts:
        draws = jax.random.uniform(jax.random.fold_in(jax.random.fold_in(rng, 6), dim), (parts,), jnp.float32, smallest / len(cuts), largest / len(cuts))
        factor_of = factor_of * jnp.repeat(jnp.exp(draws), shape[dim] // parts).reshape((-1,) + (1,) * (len(shape) - 1 - dim))
    return factor_of


def bell_draw(rng, shape, scale, reach, cuts=(), kind=jnp.bfloat16):
    factor_of = levels(rng, shape, cuts, -0.22, 0.18) if cuts else 1.0
    array = jax.random.normal(rng, shape, jnp.float32) * scale * factor_of
    return jnp.minimum(jnp.maximum(array, -reach), reach).astype(kind)


def setup_inputs(seed: int = 0, part: int = 0) -> dict:
    splits = jax.random.split(jax.random.key(seed), 8)
    own_keys = jax.random.split(jax.random.fold_in(splits[7], part), 8)
    queries = draw_queries(jax.random.fold_in(jax.random.fold_in(splits[7], part), 71), part)
    keys = draw_keys(jax.random.fold_in(jax.random.fold_in(splits[7], part), 71), part)
    values = bell_draw(own_keys[2], (TOKENS, HEADS * HEAD_DIM), 1.0, 6.0, ((0, 128),))
    block_counts = draw_block_counts(jax.random.fold_in(jax.random.fold_in(splits[7], part), 71), part)
    last_tokens = touch_ends(jax.random.randint(own_keys[4], (2 * PAIRS,), BLOCK // 2, BLOCK + 1), jax.random.fold_in(own_keys[4], 1), BLOCK // 2, BLOCK).astype(jnp.int32)
    pack_order = draw_pack_order(jax.random.fold_in(jax.random.fold_in(splits[7], part), 71), part)
    decode_slot = jax.random.permutation(own_keys[6], PAIRS).astype(jnp.int32)
    return {"queries": queries, "keys": keys, "values": values, "block_counts": block_counts, "last_tokens": last_tokens, "pack_order": pack_order, "decode_slot": decode_slot}


MASKED_SCORE = -1.0e30


def block_tables(block_counts, last_tokens, pack_order, decode_slot, total_blocks, block):
    pair_count = block_counts.shape[0]
    prompts = 2 * pair_count
    prompt_ids = jnp.arange(prompts, dtype=jnp.int32)
    prompt_sizes = jnp.concatenate([block_counts, jnp.ones((pair_count,), jnp.int32)])
    picked = (pack_order[:, None] == prompt_ids[None, :]).astype(jnp.int32)
    packed_sizes = jnp.sum(picked * prompt_sizes[None, :], axis=1).astype(jnp.int32)
    packed_tails = jnp.sum(picked * last_tokens[None, :], axis=1).astype(jnp.int32)
    block_ends = jnp.cumsum(packed_sizes).astype(jnp.int32)
    starts = block_ends - packed_sizes
    blocks = jnp.arange(total_blocks, dtype=jnp.int32)
    member = ((starts[None, :] <= blocks[:, None]) & (blocks[:, None] < block_ends[None, :])).astype(jnp.int32)
    position = jnp.sum(member * prompt_ids[None, :], axis=1).astype(jnp.int32)
    prompt = jnp.sum(member * pack_order[None, :], axis=1).astype(jnp.int32)
    within = blocks - jnp.sum(member * starts[None, :], axis=1).astype(jnp.int32)
    is_last = (blocks + 1) == jnp.sum(member * block_ends[None, :], axis=1).astype(jnp.int32)
    valid_tokens = jnp.where(is_last, jnp.sum(member * packed_tails[None, :], axis=1).astype(jnp.int32), block).astype(jnp.int32)
    pair_ids = jnp.arange(pair_count, dtype=jnp.int32)
    earlier = (decode_slot[None, :] < decode_slot[:, None]).astype(jnp.int32)
    slot_start = jnp.sum(earlier * (block_counts + 1)[None, :], axis=1).astype(jnp.int32)
    pair_of = prompt % pair_count
    owner = (pair_of[:, None] == pair_ids[None, :]).astype(jnp.int32)
    base_slot = jnp.sum(owner * slot_start[None, :], axis=1).astype(jnp.int32)
    own_count = jnp.sum(owner * block_counts[None, :], axis=1).astype(jnp.int32)
    destination = base_slot + jnp.where(prompt >= pair_count, own_count, within)
    hits = (destination[None, :] == blocks[:, None]).astype(jnp.int32)
    source = jnp.sum(hits * blocks[None, :], axis=1).astype(jnp.int32)
    return position, valid_tokens, source


def reference(queries, keys, values, block_counts, last_tokens, pack_order, decode_slot):
    position, valid_tokens, source = block_tables(block_counts, last_tokens, pack_order, decode_slot, NB, BLOCK)
    features = HEADS * HEAD_DIM
    back = MAXB - 1
    span = (back + 1) * BLOCK
    padding = jnp.zeros((back * BLOCK, features), jnp.bfloat16)
    padded_keys = jnp.concatenate([padding, keys], axis=0)
    padded_values = jnp.concatenate([padding, values], axis=0)
    padded_docs = jnp.concatenate([jnp.full((back,), -1, jnp.int32), position])
    padded_valid = jnp.concatenate([jnp.zeros((back,), jnp.int32), valid_tokens])
    token_ids = jnp.arange(BLOCK, dtype=jnp.int32)
    key_blocks = jnp.repeat(jnp.arange(back + 1, dtype=jnp.int32), BLOCK)
    key_tokens = jnp.tile(token_ids, back + 1)
    score_scale = HEAD_DIM ** -0.5

    def one_block(block_index):
        start = (block_index * BLOCK).astype(jnp.int32)
        key_window = lax.dynamic_slice_in_dim(padded_keys, start, span, 0).reshape(span, HEADS, HEAD_DIM)
        value_window = lax.dynamic_slice_in_dim(padded_values, start, span, 0).reshape(span, HEADS, HEAD_DIM)
        window_docs = lax.dynamic_slice_in_dim(padded_docs, block_index, back + 1)
        window_valid = lax.dynamic_slice_in_dim(padded_valid, block_index, back + 1)
        query_block = lax.dynamic_slice_in_dim(queries, start, BLOCK, 0).reshape(BLOCK, HEADS, HEAD_DIM)
        own_doc = window_docs[back]
        own_valid = window_valid[back]
        key_ok = (jnp.repeat(window_docs, BLOCK) == own_doc) & (key_tokens < jnp.repeat(window_valid, BLOCK))
        causal = (key_blocks[None, :] < back) | (key_tokens[None, :] <= token_ids[:, None])
        allowed = causal & key_ok[None, :]
        scores = jnp.einsum("qhd,khd->hqk", query_block.astype(jnp.float32), key_window.astype(jnp.float32)) * score_scale
        scores = jnp.where(allowed[None], scores, MASKED_SCORE)
        peak = jnp.max(scores, axis=2, keepdims=True)
        weights = jnp.exp(scores - peak)
        totals = jnp.sum(weights, axis=2, keepdims=True)
        rounded = lax.optimization_barrier(weights.astype(jnp.bfloat16)).astype(jnp.float32)
        mixed = jnp.einsum("hqk,khd->hqd", rounded, value_window.astype(jnp.float32)) / totals
        mixed = jnp.where((token_ids < own_valid)[None, :, None], mixed, 0.0)
        return jnp.transpose(mixed, (1, 0, 2)).reshape(BLOCK, features).astype(jnp.bfloat16)

    attended = lax.map(one_block, jnp.arange(NB, dtype=jnp.int32)).reshape(TOKENS, features)

    def relayout(source_array):
        grid = source_array.reshape(NB, SPLITS, SLICE, HEADS, HEAD_DIM)
        reordered = jnp.take(grid, source, axis=0)
        return jnp.transpose(reordered, (3, 1, 0, 2, 4)).reshape(HEADS * SPLITS, NB, SLICE, HEAD_DIM)

    return attended, relayout(keys), relayout(values)
```

```python
import functools

import jax
import jax.numpy as jnp
from jax import lax
from jax.experimental import pallas as pl
from jax.experimental.pallas import tpu as pltpu
from jax.sharding import PartitionSpec as P

HEADS = 16
HEAD_DIM = 128
BLOCK = 128
MAXB = 6
PRIOR = MAXB - 1
MASKED_SCORE = -1e30
MESH = pl.DeviceIdType.MESH
BF16 = jnp.bfloat16
F32 = jnp.float32


def column(row):
    n = row.shape[1]
    diagonal = lax.broadcasted_iota(jnp.int32, (n, n), 0) == lax.broadcasted_iota(jnp.int32, (n, n), 1)
    return jnp.sum(jnp.where(diagonal, row, 0), axis=1, keepdims=True)


def pick(mask, values):
    return jnp.sum(jnp.where(mask, values, 0), axis=0, keepdims=True)


def block_tables(counts_ref, tails_ref, order_ref, slots_ref, rows_ref, table_ref):
    pairs = counts_ref.shape[1]
    prompts = order_ref.shape[1]
    blocks = table_ref.shape[1]

    def iota(shape, axis):
        return lax.broadcasted_iota(jnp.int32, shape, axis)

    rows_ref[0:1, :] = jnp.zeros((1, prompts), jnp.int32)
    rows_ref[1:2, :] = jnp.ones((1, prompts), jnp.int32)
    rows_ref[2:3, :] = jnp.full((1, prompts), 1 << 20, jnp.int32)
    rows_ref[0:1, 0:pairs] = counts_ref[...]
    rows_ref[1:2, 0:pairs] = counts_ref[...]
    rows_ref[2:3, 0:pairs] = slots_ref[...]
    counts = rows_ref[0:1, :]
    sizes = rows_ref[1:2, :]
    slots = rows_ref[2:3, :]
    order = order_ref[...]
    tails = tails_ref[...]

    square = (prompts, prompts)
    picked = iota(square, 0) == order
    packed_sizes = pick(picked, column(sizes))
    packed_tails = pick(picked, column(tails))
    ends = pick(iota(square, 0) <= iota(square, 1), column(packed_sizes))
    starts = ends - packed_sizes

    wide = (prompts, blocks)
    block = iota((1, blocks), 1)
    ends_column = column(ends)
    starts_column = column(starts)
    member = (starts_column <= block) & (block < ends_column)
    position = pick(member, iota(wide, 0))
    prompt = pick(member, column(order))
    within = block - pick(member, starts_column)
    last = block + 1 == pick(member, ends_column)
    valid = jnp.where(last, pick(member, column(packed_tails)), BLOCK)

    slot_start = pick(column(slots) < slots, column(counts) + 1)
    null = prompt >= pairs
    owner = iota(wide, 0) == jnp.where(null, prompt - pairs, prompt)
    destination = pick(owner, column(slot_start)) + jnp.where(null, pick(owner, column(counts)), within)
    full = (blocks, blocks)
    source = jnp.minimum(pick(column(destination) == iota(full, 1), iota(full, 0)), blocks - 1)

    table_ref[0:1, :] = position
    table_ref[1:2, :] = valid
    table_ref[2:3, :] = source


def exchange_kernel(
    rows,
    cols,
    q_ref,
    k_ref,
    v_ref,
    counts_ref,
    tails_ref,
    order_ref,
    slots_ref,
    att_ref,
    out_k,
    out_v,
    win,
    q_vmem,
    stage,
    cross,
    recv,
    allowed,
    small_rows,
    table_vmem,
    table,
    load_sem,
    table_sem,
    halo_sem,
    halo_send,
    cross_sem,
    cross_send,
    relay_send,
    z_send,
    z_sem,
    row_send,
    row_sem,
    lower_ready,
    upper_ready,
):
    me = lax.axis_index("seq")
    z = me // cols
    i = lax.rem(me, cols)
    x = i // 2
    core = lax.rem(i, 2)
    own = PRIOR
    here = win.shape[1] - PRIOR
    group = win.shape[3] // (cols // 2)
    part = BLOCK // cols

    def device(row, place):
        return {"seq": row * cols + place}

    def send(src, dst, ssem, rsem, target):
        return pltpu.make_async_remote_copy(
            src_ref=src, dst_ref=dst, send_sem=ssem, recv_sem=rsem, device_id=target, device_id_type=MESH
        )

    loads = [
        pltpu.make_async_copy(k_ref, win.at[0, pl.ds(own, here)], load_sem.at[0]),
        pltpu.make_async_copy(v_ref, win.at[1, pl.ds(own, here)], load_sem.at[1]),
        pltpu.make_async_copy(q_ref, q_vmem, load_sem.at[2]),
    ]
    for load in loads:
        load.start()

    barrier = pltpu.get_barrier_semaphore()

    def greet_row(row, first):
        def greet(k, carry):
            place = lax.rem(i + k, cols)
            pl.semaphore_signal(barrier, inc=1, device_id=device(row, place), device_id_type=MESH)
            return carry

        lax.fori_loop(first, cols, greet, 0)

    greet_row(z, 1)

    @pl.when(z > 0)
    def _():
        greet_row(z - 1, 0)

    @pl.when(z < rows - 1)
    def _():
        greet_row(z + 1, 0)

    for load in loads:
        load.wait()
    next_rows = jnp.where(z > 0, cols, 0) + jnp.where(z < rows - 1, cols, 0)
    pl.semaphore_wait(barrier, cols - 1 + next_rows)

    spans = {cols - 1: (PRIOR - 2, 2), cols - 2: (PRIOR - 4, 2), cols - 3: (0, 1)}
    has_next = z < rows - 1

    def columns_of(g):
        return pl.ds(pl.multiple_of(g * group, group), group)

    def crossing(place, g):
        first, length = spans[place]
        n = place - (cols - 3)
        src = win.at[:, pl.ds(own + here - length, length), :, columns_of(g)]
        if place // 2 == g:
            return send(
                src,
                win.at[:, pl.ds(first, length), :, columns_of(g)],
                cross_send.at[n, g],
                halo_sem.at[0 if place == cols - 1 else 1],
                device(z + 1, 0),
            )
        return send(
            src, cross.at[:, pl.ds(first, length)], cross_send.at[n, g], cross_sem.at[n], device(z, 2 * g + 1)
        )

    for place in spans:

        @pl.when(has_next & (i == place))
        def _(place=place):
            for g in range(cols // 2):
                crossing(place, g).start()

    def next_odd():
        return send(
            win.at[:, pl.ds(own, here)],
            win.at[:, pl.ds(PRIOR - here, here)],
            halo_send.at[0],
            halo_sem.at[0],
            device(z, i + 1),
        )

    def next_even():
        return send(
            win.at[:, pl.ds(own, here)],
            win.at[:, pl.ds(PRIOR - 2 * here, here)],
            halo_send.at[1],
            halo_sem.at[1],
            device(z, i + 2),
        )

    def pass_last():
        return send(
            win.at[:, pl.ds(PRIOR - 1, 1)],
            win.at[:, pl.ds(0, 1)],
            halo_send.at[2],
            halo_sem.at[1],
            device(z, i + 2),
        )

    def pass_pair():
        return send(
            win.at[:, pl.ds(PRIOR - here, here)],
            win.at[:, pl.ds(PRIOR - 2 * here, here)],
            halo_send.at[3],
            halo_sem.at[1],
            device(z, i + 1),
        )

    def pass_single():
        return send(
            win.at[:, pl.ds(PRIOR - here - 1, 1)],
            win.at[:, pl.ds(0, 1)],
            halo_send.at[4],
            halo_sem.at[1],
            device(z, i + 1),
        )

    even = core == 0
    has_two_on = even & (i < cols - 2)

    @pl.when(i < cols - 1)
    def _():
        next_odd().start()

    @pl.when(has_two_on)
    def _():
        next_even().start()

    @pl.when(me == 0)
    def _():
        for n, ref in enumerate((k_ref, v_ref)):
            pltpu.make_async_copy(ref, win.at[n, pl.ds(PRIOR - here, here)], halo_sem.at[0]).start()
            pltpu.make_async_copy(ref, win.at[n, pl.ds(PRIOR - 2 * here, here)], halo_sem.at[1]).start()
            pltpu.make_async_copy(ref.at[pl.ds(0, 1)], win.at[n, pl.ds(0, 1)], halo_sem.at[1]).start()

    def head_columns(row):
        return pl.ds(pl.multiple_of(row * HEAD_DIM, HEAD_DIM), HEAD_DIM)

    def slice_of(place):
        return pl.ds(pl.multiple_of(place * part, part), part)

    def blocks_of(row):
        return pl.ds((row * cols + i) * here, here)

    def give_own(k, carry):
        place = lax.rem(i + k, cols)
        send(
            win.at[:, pl.ds(own, here), slice_of(place), head_columns(z)],
            recv.at[:, blocks_of(z)],
            row_send,
            row_sem,
            device(z, place),
        ).start()
        return carry

    lax.fori_loop(1, cols, give_own, 0)
    recv[:, blocks_of(z)] = win[:, own : own + here, slice_of(i), head_columns(z)]

    @pl.when(z > 0)
    def _():
        pl.semaphore_wait(lower_ready, 1)

    @pl.when(z < rows - 1)
    def _():
        pl.semaphore_signal(lower_ready, inc=1, device_id=device(z + 1, i), device_id_type=MESH)

    def tell(row, carry):
        pl.semaphore_signal(upper_ready.at[z], inc=1, device_id=device(row, i), device_id_type=MESH)
        return carry

    lax.fori_loop(0, z, tell, 0)

    def give_head(row):
        send(
            win.at[:, pl.ds(own, here), :, head_columns(row)],
            stage.at[z],
            z_send,
            z_sem.at[z],
            device(row, i),
        ).start()

    def give_below(k, carry):
        give_head(z - k)
        return carry

    half = rows // 2
    near = jnp.minimum(z, half)
    lax.fori_loop(1, near + 1, give_below, 0)

    def relay(place):
        first, length = spans[place]
        return send(
            cross.at[:, pl.ds(first, length)],
            win.at[:, pl.ds(first, length), :, columns_of(x)],
            relay_send.at[place - (cols - 3)],
            halo_sem.at[0 if place == cols - 1 else 1],
            device(z + 1, 0),
        )

    for place in spans:

        @pl.when(has_next & (core == 1) & (x != place // 2))
        def _(place=place):
            first, length = spans[place]
            span = cross.at[:, pl.ds(first, length)]
            pltpu.make_async_copy(span, span, cross_sem.at[place - (cols - 3)]).wait()
            relay(place).start()

    lax.fori_loop(near + 1, z + 1, give_below, 0)

    def give_above(row, carry):
        pl.semaphore_wait(upper_ready.at[row], 1)
        give_head(row)
        return carry

    lax.fori_loop(z + 1, rows, give_above, 0)

    block_tables(counts_ref, tails_ref, order_ref, slots_ref, small_rows, table_vmem)

    def arrived(step):
        k = step // 2 + 1
        row = lax.rem(z + jnp.where(lax.rem(step, 2) == 0, k, rows - k), rows)
        pltpu.make_async_copy(stage.at[row], stage.at[row], z_sem.at[row]).wait()

        def give(n, carry):
            place = lax.rem(i + n, cols)
            send(
                stage.at[row, :, :, slice_of(place), :],
                recv.at[:, blocks_of(row)],
                row_send,
                row_sem,
                device(z, place),
            ).start()
            return carry

        lax.fori_loop(1, cols, give, 0)
        recv[:, blocks_of(row)] = stage[row, :, :, slice_of(i), :]

    early = (rows - 1) // 2

    def early_step(step, carry):
        arrived(step)
        return carry

    lax.fori_loop(0, early, early_step, 0)

    table_copy = pltpu.make_async_copy(table_vmem, table, table_sem)
    table_copy.start()
    table_copy.wait()

    late_half = win.at[:, pl.ds(PRIOR - here, here)]
    pltpu.make_async_copy(late_half, late_half, halo_sem.at[0]).wait()

    @pl.when(has_two_on)
    def _():
        pass_last().start()

    @pl.when(even)
    def _():
        pass_pair().start()

    early_half = win.at[:, pl.ds(0, PRIOR - here)]
    pltpu.make_async_copy(early_half, early_half, halo_sem.at[1]).wait()

    @pl.when(even)
    def _():
        pass_single().start()

    tokens = here * BLOCK
    span = MAXB * BLOCK - BLOCK + tokens
    query = lax.broadcasted_iota(jnp.int32, (tokens, BLOCK), 0)
    query_block = query // BLOCK
    token = lax.broadcasted_iota(jnp.int32, (tokens, BLOCK), 1)
    first_block = me * here
    query_doc = jnp.zeros((tokens, BLOCK), jnp.int32)
    query_valid = jnp.zeros((tokens, BLOCK), jnp.int32)
    for b in range(here):
        query_doc = jnp.where(query_block == b, table[0, first_block + b], query_doc)
        query_valid = jnp.where(query_block == b, table[1, first_block + b], query_valid)
    query_ok = lax.rem(query, BLOCK) < query_valid
    for b in range(PRIOR + here):
        block = first_block + b - PRIOR
        there = jnp.maximum(block, 0)
        doc = jnp.where(block >= 0, table[0, there], -1)
        limit = jnp.where(block >= 0, table[1, there], 0)
        seen = (query_doc == doc) & (token < limit) & (token + (b - PRIOR) * BLOCK <= query)
        allowed[:, b * BLOCK : (b + 1) * BLOCK] = seen.astype(F32)

    def attend(head):
        at = head_columns(head)
        keys = win[0, :, :, at].reshape(span, HEAD_DIM)
        values = win[1, :, :, at].reshape(span, HEAD_DIM)
        scores = lax.dot_general(
            q_vmem[:, at], keys, (((1,), (1,)), ((), ())), preferred_element_type=F32
        ) * (HEAD_DIM**-0.5)
        scores = jnp.where(allowed[...] > 0.5, scores, MASKED_SCORE)
        peak = jnp.max(scores, axis=1, keepdims=True)
        weights = jnp.exp(scores - peak)
        totals = jnp.sum(weights, axis=1, keepdims=True)
        mixed = jnp.dot(weights.astype(BF16), values, preferred_element_type=F32)
        att_ref[:, at] = jnp.where(query_ok, mixed / totals, 0.0).astype(BF16)

    per_step = HEADS // (rows - 1 - early)

    def late_step(step, carry):
        def one(n, c):
            attend((step - early) * per_step + n)
            return c

        lax.fori_loop(0, per_step, one, 0)
        arrived(step)
        return carry

    lax.fori_loop(early, rows - 1, late_step, 0)

    def rest(head, carry):
        attend(head)
        return carry

    lax.fori_loop(per_step * (rows - 1 - early), HEADS, rest, 0)

    landed = recv.at[:, pl.ds(0, rows * (cols - 1) * here)]
    pltpu.make_async_copy(landed, landed, row_sem).wait()

    def place_block(c, carry):
        s = jnp.clip(table[2, c], 0, out_k.shape[0] - 1)
        out_k[c] = recv[0, s]
        out_v[c] = recv[1, s]
        return carry

    lax.fori_loop(0, out_k.shape[0], place_block, 0, unroll=8)

    pltpu.make_async_copy(landed, landed, row_send).wait()
    heads_sent = stage.at[pl.ds(0, rows - 1)]
    pltpu.make_async_copy(heads_sent, heads_sent, z_send).wait()
    for place in spans:

        @pl.when(has_next & (i == place))
        def _(place=place):
            for g in range(cols // 2):
                crossing(place, g).wait_send()

        @pl.when(has_next & (core == 1) & (x != place // 2))
        def _(place=place):
            relay(place).wait_send()

    @pl.when(i < cols - 1)
    def _():
        next_odd().wait_send()

    @pl.when(has_two_on)
    def _():
        next_even().wait_send()
        pass_last().wait_send()

    @pl.when(even)
    def _():
        pass_pair().wait_send()
        pass_single().wait_send()


def local(queries, keys, values, block_counts, last_tokens, pack_order, decode_slot):
    devices = lax.axis_size("seq")
    tokens, features = queries.shape
    here = tokens // BLOCK
    cols = devices // HEADS
    rows = HEADS
    blocks = devices * here
    part = BLOCK // cols
    prompts = pack_order.shape[0]
    window = PRIOR + here
    hbm = pl.BlockSpec(memory_space=pltpu.HBM)
    vmem = pl.BlockSpec(memory_space=pltpu.VMEM)
    dma = pltpu.SemaphoreType.DMA
    regular = pltpu.SemaphoreType.REGULAR
    shapes = ((tokens, features), (blocks, part, HEAD_DIM), (blocks, part, HEAD_DIM))
    attended, cache_keys, cache_values = pl.pallas_call(
        functools.partial(exchange_kernel, rows, cols),
        out_shape=[pltpu.VMEM(shape, BF16) for shape in shapes],
        in_specs=[hbm] * 3 + [vmem] * 4,
        out_specs=[vmem] * 3,
        scratch_shapes=[
            pltpu.VMEM((2, window, BLOCK, features), BF16),
            pltpu.VMEM((tokens, features), BF16),
            pltpu.VMEM((rows, 2, here, BLOCK, HEAD_DIM), BF16),
            pltpu.VMEM((2, PRIOR, BLOCK, features // (cols // 2)), BF16),
            pltpu.VMEM((2, blocks, part, HEAD_DIM), BF16),
            pltpu.VMEM((tokens, window * BLOCK), F32),
            pltpu.VMEM((8, prompts), jnp.int32),
            pltpu.VMEM((8, blocks), jnp.int32),
            pltpu.SMEM((8, blocks), jnp.int32),
            dma((3,)),
            dma,
            dma((2,)),
            dma((5,)),
            dma((3,)),
            dma((3, cols // 2)),
            dma((3,)),
            dma,
            dma((rows,)),
            dma,
            dma,
            regular,
            regular((rows,)),
        ],
        compiler_params=pltpu.CompilerParams(
            collective_id=0, has_side_effects=True, vmem_limit_bytes=60 * 1024 * 1024
        ),
    )(
        queries,
        keys.reshape(here, BLOCK, features),
        values.reshape(here, BLOCK, features),
        block_counts.reshape(1, -1),
        last_tokens.reshape(1, -1),
        pack_order.reshape(1, -1),
        decode_slot.reshape(1, -1),
    )
    return (attended, cache_keys[None], cache_values[None])


def solution(mesh):
    placed = (P(("groups", "seq"), None),) * 3 + (P("groups"),) * 4
    return jax.shard_map(
        local,
        mesh=mesh,
        in_specs=placed,
        out_specs=(
            P(("groups", "seq"), None),
            P(("groups", "seq"), None, None, None),
            P(("groups", "seq"), None, None, None),
        ),
        check_vma=False,
    )
```

```python
import functools

import jax
import jax.numpy as jnp
from jax import lax
from jax.experimental import pallas as pl
from jax.experimental.pallas import tpu as pltpu
from jax.sharding import PartitionSpec as P

HEADS = 16
HEAD_DIM = 128
BLOCK = 128
MAXB = 6
PRIOR = MAXB - 1
MASKED_SCORE = -1e30
MESH = pl.DeviceIdType.MESH
BF16 = jnp.bfloat16
F32 = jnp.float32


def column(row):
    n = row.shape[1]
    diagonal = lax.broadcasted_iota(jnp.int32, (n, n), 0) == lax.broadcasted_iota(jnp.int32, (n, n), 1)
    return jnp.sum(jnp.where(diagonal, row, 0), axis=1, keepdims=True)


def pick(mask, values):
    return jnp.sum(jnp.where(mask, values, 0), axis=0, keepdims=True)


def block_tables(counts_ref, tails_ref, order_ref, slots_ref, rows_ref, table_ref):
    pairs = counts_ref.shape[1]
    prompts = order_ref.shape[1]
    blocks = table_ref.shape[1]

    def iota(shape, axis):
        return lax.broadcasted_iota(jnp.int32, shape, axis)

    rows_ref[0:1, :] = jnp.zeros((1, prompts), jnp.int32)
    rows_ref[1:2, :] = jnp.ones((1, prompts), jnp.int32)
    rows_ref[2:3, :] = jnp.full((1, prompts), 1 << 20, jnp.int32)
    rows_ref[0:1, 0:pairs] = counts_ref[...]
    rows_ref[1:2, 0:pairs] = counts_ref[...]
    rows_ref[2:3, 0:pairs] = slots_ref[...]
    counts = rows_ref[0:1, :]
    sizes = rows_ref[1:2, :]
    slots = rows_ref[2:3, :]
    order = order_ref[...]
    tails = tails_ref[...]

    square = (prompts, prompts)
    picked = iota(square, 0) == order
    packed_sizes = pick(picked, column(sizes))
    packed_tails = pick(picked, column(tails))
    ends = pick(iota(square, 0) <= iota(square, 1), column(packed_sizes))
    starts = ends - packed_sizes

    wide = (prompts, blocks)
    block = iota((1, blocks), 1)
    ends_column = column(ends)
    starts_column = column(starts)
    member = (starts_column <= block) & (block < ends_column)
    position = pick(member, iota(wide, 0))
    prompt = pick(member, column(order))
    within = block - pick(member, starts_column)
    last = block + 1 == pick(member, ends_column)
    valid = jnp.where(last, pick(member, column(packed_tails)), BLOCK)

    slot_start = pick(column(slots) < slots, column(counts) + 1)
    null = prompt >= pairs
    owner = iota(wide, 0) == jnp.where(null, prompt - pairs, prompt)
    destination = pick(owner, column(slot_start)) + jnp.where(null, pick(owner, column(counts)), within)
    full = (blocks, blocks)
    source = jnp.minimum(pick(column(destination) == iota(full, 1), iota(full, 0)), blocks - 1)

    table_ref[0:1, :] = position
    table_ref[1:2, :] = valid
    table_ref[2:3, :] = source


def exchange_kernel(
    rows,
    cols,
    q_ref,
    k_ref,
    v_ref,
    counts_ref,
    tails_ref,
    order_ref,
    slots_ref,
    att_ref,
    out_k,
    out_v,
    win,
    q_vmem,
    cross,
    recv,
    allowed,
    counts,
    tails,
    order,
    slots,
    small_rows,
    table_vmem,
    table,
    load_sem,
    table_sem,
    halo_sem,
    halo_send,
    cross_sem,
    cross_send,
    relay_send,
    row_send,
    row_sem,
    lower_ready,
    upper_ready,
):
    me = lax.axis_index("seq")
    z = me // cols
    i = lax.rem(me, cols)
    x = i // 2
    core = lax.rem(i, 2)
    own = PRIOR
    here = win.shape[1] - PRIOR
    group = win.shape[3] // (cols // 2)
    part = BLOCK // cols

    def device(row, place):
        return {"seq": row * cols + place}

    def send(src, dst, ssem, rsem, target):
        return pltpu.make_async_remote_copy(
            src_ref=src, dst_ref=dst, send_sem=ssem, recv_sem=rsem, device_id=target, device_id_type=MESH
        )

    loads = [
        pltpu.make_async_copy(k_ref, win.at[0, pl.ds(own, here)], load_sem.at[0]),
        pltpu.make_async_copy(v_ref, win.at[1, pl.ds(own, here)], load_sem.at[1]),
    ]
    later = [
        pltpu.make_async_copy(src, dst, load_sem.at[2 + n])
        for n, (src, dst) in enumerate(
            (
                (q_ref, q_vmem),
                (counts_ref, counts),
                (tails_ref, tails),
                (order_ref, order),
                (slots_ref, slots),
            )
        )
    ]

    barrier = pltpu.get_barrier_semaphore()

    def greet(row, place):
        pl.semaphore_signal(barrier, inc=1, device_id=device(row, place), device_id_type=MESH)

    def greet_row(k, carry):
        greet(z, lax.rem(i + k, cols))
        return carry

    lax.fori_loop(1, cols, greet_row, 0)
    line = lax.rem(z + rows - 1, rows)
    line_first, line_last = line == 0, line == rows - 1

    def row_at(place):
        return lax.rem(place + 1, rows)

    @pl.when(jnp.logical_not(line_first))
    def _():
        greet(row_at(line - 1), i)

    @pl.when(jnp.logical_not(line_last))
    def _():
        greet(row_at(line + 1), i)

    has_next = z < rows - 1
    senders = [place for place in range(cols) if place % 2 == 1 or place >= cols - 3]
    crosses = core == 1
    for place in senders:
        crosses = crosses | (i == place)
    crosses = crosses & has_next
    receives = (i == 0) & (z > 0)

    @pl.when(crosses)
    def _():
        greet(z + 1, 0)

    @pl.when(receives)
    def _():
        for place in senders:
            greet(z - 1, place)

    for load in loads + later:
        load.start()
    peers = cols - 1 + jnp.where(line_first, 0, 1) + jnp.where(line_last, 0, 1)
    pl.semaphore_wait(barrier, peers + jnp.where(crosses, 1, 0) + jnp.where(receives, len(senders), 0))
    for load in loads:
        load.wait()

    spans = {cols - 1: (PRIOR - 2, 2), cols - 2: (PRIOR - 4, 2), cols - 3: (0, 1)}
    def columns_of(g):
        return pl.ds(pl.multiple_of(g * group, group), group)

    def crossing(place, g):
        first, length = spans[place]
        n = place - (cols - 3)
        src = win.at[:, pl.ds(own + here - length, length), :, columns_of(g)]
        if place // 2 == g:
            return send(
                src,
                win.at[:, pl.ds(first, length), :, columns_of(g)],
                cross_send.at[n, g],
                halo_sem.at[0 if place == cols - 1 else 1],
                device(z + 1, 0),
            )
        return send(
            src, cross.at[:, pl.ds(first, length)], cross_send.at[n, g], cross_sem.at[n], device(z, 2 * g + 1)
        )

    for place in spans:

        @pl.when(has_next & (i == place))
        def _(place=place):
            for g in range(cols // 2):
                crossing(place, g).start()

    def next_odd():
        return send(
            win.at[:, pl.ds(own, here)],
            win.at[:, pl.ds(PRIOR - here, here)],
            halo_send.at[0],
            halo_sem.at[0],
            device(z, i + 1),
        )

    def next_even():
        return send(
            win.at[:, pl.ds(own, here)],
            win.at[:, pl.ds(PRIOR - 2 * here, here)],
            halo_send.at[1],
            halo_sem.at[1],
            device(z, i + 2),
        )

    def pass_last():
        return send(
            win.at[:, pl.ds(PRIOR - 1, 1)],
            win.at[:, pl.ds(0, 1)],
            halo_send.at[2],
            halo_sem.at[1],
            device(z, i + 2),
        )

    def pass_pair():
        return send(
            win.at[:, pl.ds(PRIOR - here, here)],
            win.at[:, pl.ds(PRIOR - 2 * here, here)],
            halo_send.at[3],
            halo_sem.at[1],
            device(z, i + 1),
        )

    def pass_single():
        return send(
            win.at[:, pl.ds(PRIOR - here - 1, 1)],
            win.at[:, pl.ds(0, 1)],
            halo_send.at[4],
            halo_sem.at[1],
            device(z, i + 1),
        )

    even = core == 0
    has_two_on = even & (i < cols - 2)

    @pl.when(i < cols - 1)
    def _():
        next_odd().start()

    @pl.when(has_two_on)
    def _():
        next_even().start()

    @pl.when(me == 0)
    def _():
        for n, ref in enumerate((k_ref, v_ref)):
            pltpu.make_async_copy(ref, win.at[n, pl.ds(PRIOR - here, here)], halo_sem.at[0]).start()
            pltpu.make_async_copy(ref, win.at[n, pl.ds(PRIOR - 2 * here, here)], halo_sem.at[1]).start()
            pltpu.make_async_copy(ref.at[pl.ds(0, 1)], win.at[n, pl.ds(0, 1)], halo_sem.at[1]).start()

    def head_columns(row):
        return pl.ds(pl.multiple_of(row * HEAD_DIM, HEAD_DIM), HEAD_DIM)

    def slice_of(place):
        return pl.ds(pl.multiple_of(place * part, part), part)

    mine = pl.ds(me * here, here)

    def give_own(k, carry):
        place = lax.rem(i + k, cols)
        send(
            win.at[:, pl.ds(own, here), slice_of(place), head_columns(z)],
            recv.at[:, mine],
            row_send,
            row_sem,
            device(z, place),
        ).start()
        return carry

    lax.fori_loop(1, cols, give_own, 0)
    recv[:, mine] = win[:, own : own + here, slice_of(i), head_columns(z)]

    @pl.when(jnp.logical_not(line_first))
    def _():
        pl.semaphore_wait(lower_ready, 1)

    @pl.when(jnp.logical_not(line_last))
    def _():
        pl.semaphore_signal(lower_ready, inc=1, device_id=device(row_at(line + 1), i), device_id_type=MESH)

    def tell(place, carry):
        pl.semaphore_signal(
            upper_ready.at[line], inc=1, device_id=device(row_at(place), i), device_id_type=MESH
        )
        return carry

    lax.fori_loop(0, line, tell, 0)

    def give_row(row):
        def give(k, carry):
            place = lax.rem(i + k, cols)
            send(
                win.at[:, pl.ds(own, here), slice_of(place), head_columns(row)],
                recv.at[:, mine],
                row_send,
                row_sem,
                device(row, place),
            ).start()
            return carry

        lax.fori_loop(0, cols, give, 0)

    def give_below(k, carry):
        give_row(row_at(line - k))
        return carry

    near = jnp.minimum(line, rows // 2)

    def give_near(k, carry):
        give_row(row_at(line - near + k))
        return carry

    lax.fori_loop(0, near, give_near, 0)

    def relay(place):
        first, length = spans[place]
        return send(
            cross.at[:, pl.ds(first, length)],
            win.at[:, pl.ds(first, length), :, columns_of(x)],
            relay_send.at[place - (cols - 3)],
            halo_sem.at[0 if place == cols - 1 else 1],
            device(z + 1, 0),
        )

    for place in spans:

        @pl.when(has_next & (core == 1) & (x != place // 2))
        def _(place=place):
            first, length = spans[place]
            span = cross.at[:, pl.ds(first, length)]
            pltpu.make_async_copy(span, span, cross_sem.at[place - (cols - 3)]).wait()
            relay(place).start()

    lax.fori_loop(near + 1, line + 1, give_below, 0)

    def give_above(place, carry):
        pl.semaphore_wait(upper_ready.at[place], 1)
        give_row(row_at(place))
        return carry

    lax.fori_loop(line + 1, rows, give_above, 0)

    for load in later:
        load.wait()
    block_tables(counts, tails, order, slots, small_rows, table_vmem)

    table_copy = pltpu.make_async_copy(table_vmem, table, table_sem)
    table_copy.start()
    table_copy.wait()

    late_half = win.at[:, pl.ds(PRIOR - here, here)]
    pltpu.make_async_copy(late_half, late_half, halo_sem.at[0]).wait()

    @pl.when(has_two_on)
    def _():
        pass_last().start()

    @pl.when(even)
    def _():
        pass_pair().start()

    early_half = win.at[:, pl.ds(0, PRIOR - here)]
    pltpu.make_async_copy(early_half, early_half, halo_sem.at[1]).wait()

    @pl.when(even)
    def _():
        pass_single().start()

    tokens = here * BLOCK
    span = MAXB * BLOCK - BLOCK + tokens
    query = lax.broadcasted_iota(jnp.int32, (tokens, BLOCK), 0)
    query_block = query // BLOCK
    token = lax.broadcasted_iota(jnp.int32, (tokens, BLOCK), 1)
    first_block = me * here
    query_doc = jnp.zeros((tokens, BLOCK), jnp.int32)
    query_valid = jnp.zeros((tokens, BLOCK), jnp.int32)
    for b in range(here):
        query_doc = jnp.where(query_block == b, table[0, first_block + b], query_doc)
        query_valid = jnp.where(query_block == b, table[1, first_block + b], query_valid)
    query_ok = lax.rem(query, BLOCK) < query_valid
    for b in range(PRIOR + here):
        block = first_block + b - PRIOR
        there = jnp.maximum(block, 0)
        doc = jnp.where(block >= 0, table[0, there], -1)
        limit = jnp.where(block >= 0, table[1, there], 0)
        seen = (query_doc == doc) & (token < limit) & (token + (b - PRIOR) * BLOCK <= query)
        allowed[:, b * BLOCK : (b + 1) * BLOCK] = seen.astype(F32)

    def attend(head):
        at = head_columns(head)
        keys = win[0, :, :, at].reshape(span, HEAD_DIM)
        values = win[1, :, :, at].reshape(span, HEAD_DIM)
        scores = lax.dot_general(
            q_vmem[:, at], keys, (((1,), (1,)), ((), ())), preferred_element_type=F32
        ) * (HEAD_DIM**-0.5)
        scores = jnp.where(allowed[...] > 0.5, scores, MASKED_SCORE)
        peak = jnp.max(scores, axis=1, keepdims=True)
        weights = jnp.exp(scores - peak)
        totals = jnp.sum(weights, axis=1, keepdims=True)
        mixed = jnp.dot(weights.astype(BF16), values, preferred_element_type=F32)
        att_ref[:, at] = jnp.where(query_ok, mixed / totals, 0.0).astype(BF16)

    def attend_head(head, carry):
        attend(head)
        return carry

    lax.fori_loop(0, HEADS, attend_head, 0)

    landed = recv.at[:, pl.ds(0, (rows * cols - 1) * here)]
    pltpu.make_async_copy(landed, landed, row_sem).wait()

    def place_block(c, carry):
        s = jnp.clip(table[2, c], 0, out_k.shape[0] - 1)
        out_k[c] = recv[0, s]
        out_v[c] = recv[1, s]
        return carry

    lax.fori_loop(0, out_k.shape[0], place_block, 0, unroll=8)

    pltpu.make_async_copy(landed, landed, row_send).wait()
    for place in spans:

        @pl.when(has_next & (i == place))
        def _(place=place):
            for g in range(cols // 2):
                crossing(place, g).wait_send()

        @pl.when(has_next & (core == 1) & (x != place // 2))
        def _(place=place):
            relay(place).wait_send()

    @pl.when(i < cols - 1)
    def _():
        next_odd().wait_send()

    @pl.when(has_two_on)
    def _():
        next_even().wait_send()
        pass_last().wait_send()

    @pl.when(even)
    def _():
        pass_pair().wait_send()
        pass_single().wait_send()


def local(queries, keys, values, block_counts, last_tokens, pack_order, decode_slot):
    devices = lax.axis_size("seq")
    tokens, features = queries.shape
    here = tokens // BLOCK
    cols = devices // HEADS
    rows = HEADS
    blocks = devices * here
    part = BLOCK // cols
    prompts = pack_order.shape[0]
    window = PRIOR + here
    hbm = pl.BlockSpec(memory_space=pltpu.HBM)
    vmem = pl.BlockSpec(memory_space=pltpu.VMEM)
    dma = pltpu.SemaphoreType.DMA
    regular = pltpu.SemaphoreType.REGULAR
    shapes = ((tokens, features), (blocks, part, HEAD_DIM), (blocks, part, HEAD_DIM))
    attended, cache_keys, cache_values = pl.pallas_call(
        functools.partial(exchange_kernel, rows, cols),
        out_shape=[pltpu.VMEM(shape, BF16) for shape in shapes],
        in_specs=[hbm] * 7,
        out_specs=[vmem] * 3,
        scratch_shapes=[
            pltpu.VMEM((2, window, BLOCK, features), BF16),
            pltpu.VMEM((tokens, features), BF16),
            pltpu.VMEM((2, PRIOR, BLOCK, features // (cols // 2)), BF16),
            pltpu.VMEM((2, blocks, part, HEAD_DIM), BF16),
            pltpu.VMEM((tokens, window * BLOCK), F32),
            pltpu.VMEM((1, prompts // 2), jnp.int32),
            pltpu.VMEM((1, prompts), jnp.int32),
            pltpu.VMEM((1, prompts), jnp.int32),
            pltpu.VMEM((1, prompts // 2), jnp.int32),
            pltpu.VMEM((8, prompts), jnp.int32),
            pltpu.VMEM((8, blocks), jnp.int32),
            pltpu.SMEM((8, blocks), jnp.int32),
            dma((7,)),
            dma,
            dma((2,)),
            dma((5,)),
            dma((3,)),
            dma((3, cols // 2)),
            dma((3,)),
            dma,
            dma,
            regular,
            regular((rows,)),
        ],
        compiler_params=pltpu.CompilerParams(
            collective_id=0, has_side_effects=True, vmem_limit_bytes=60 * 1024 * 1024
        ),
    )(
        queries,
        keys.reshape(here, BLOCK, features),
        values.reshape(here, BLOCK, features),
        block_counts.reshape(1, -1),
        last_tokens.reshape(1, -1),
        pack_order.reshape(1, -1),
        decode_slot.reshape(1, -1),
    )
    return (attended, cache_keys[None], cache_values[None])


def solution(mesh):
    placed = (P(("groups", "seq"), None),) * 3 + (P("groups"),) * 4
    return jax.shard_map(
        local,
        mesh=mesh,
        in_specs=placed,
        out_specs=(
            P(("groups", "seq"), None),
            P(("groups", "seq"), None, None, None),
            P(("groups", "seq"), None, None, None),
        ),
        check_vma=False,
    )
```

```python
import functools

import jax
import jax.numpy as jnp
from jax import lax
from jax.experimental import pallas as pl
from jax.experimental.pallas import tpu as pltpu
from jax.sharding import PartitionSpec as P

HEADS = 16
HEAD_DIM = 128
BLOCK = 128
MAXB = 6
PRIOR = MAXB - 1
MASKED_SCORE = -1e30
MESH = pl.DeviceIdType.MESH
BF16 = jnp.bfloat16
F32 = jnp.float32


def column(row):
    n = row.shape[1]
    diagonal = lax.broadcasted_iota(jnp.int32, (n, n), 0) == lax.broadcasted_iota(jnp.int32, (n, n), 1)
    return jnp.sum(jnp.where(diagonal, row, 0), axis=1, keepdims=True)


def pick(mask, values):
    return jnp.sum(jnp.where(mask, values, 0), axis=0, keepdims=True)


def block_tables(counts_ref, tails_ref, order_ref, slots_ref, rows_ref, table_ref):
    pairs = counts_ref.shape[1]
    prompts = order_ref.shape[1]
    blocks = table_ref.shape[1]

    def iota(shape, axis):
        return lax.broadcasted_iota(jnp.int32, shape, axis)

    rows_ref[0:1, :] = jnp.zeros((1, prompts), jnp.int32)
    rows_ref[1:2, :] = jnp.ones((1, prompts), jnp.int32)
    rows_ref[2:3, :] = jnp.full((1, prompts), 1 << 20, jnp.int32)
    rows_ref[0:1, 0:pairs] = counts_ref[...]
    rows_ref[1:2, 0:pairs] = counts_ref[...]
    rows_ref[2:3, 0:pairs] = slots_ref[...]
    counts = rows_ref[0:1, :]
    sizes = rows_ref[1:2, :]
    slots = rows_ref[2:3, :]
    order = order_ref[...]
    tails = tails_ref[...]

    square = (prompts, prompts)
    picked = iota(square, 0) == order
    packed_sizes = pick(picked, column(sizes))
    packed_tails = pick(picked, column(tails))
    ends = pick(iota(square, 0) <= iota(square, 1), column(packed_sizes))
    starts = ends - packed_sizes

    wide = (prompts, blocks)
    block = iota((1, blocks), 1)
    ends_column = column(ends)
    starts_column = column(starts)
    member = (starts_column <= block) & (block < ends_column)
    position = pick(member, iota(wide, 0))
    prompt = pick(member, column(order))
    within = block - pick(member, starts_column)
    last = block + 1 == pick(member, ends_column)
    valid = jnp.where(last, pick(member, column(packed_tails)), BLOCK)

    slot_start = pick(column(slots) < slots, column(counts) + 1)
    null = prompt >= pairs
    owner = iota(wide, 0) == jnp.where(null, prompt - pairs, prompt)
    destination = pick(owner, column(slot_start)) + jnp.where(null, pick(owner, column(counts)), within)
    full = (blocks, blocks)
    source = jnp.minimum(pick(column(destination) == iota(full, 1), iota(full, 0)), blocks - 1)

    table_ref[0:1, :] = position
    table_ref[1:2, :] = valid
    table_ref[2:3, :] = source


def exchange_kernel(
    rows,
    cols,
    q_ref,
    k_ref,
    v_ref,
    counts_ref,
    tails_ref,
    order_ref,
    slots_ref,
    att_ref,
    out_k,
    out_v,
    win,
    q_vmem,
    cross,
    recv,
    allowed,
    counts,
    tails,
    order,
    slots,
    small_rows,
    table_vmem,
    table,
    load_sem,
    table_sem,
    halo_sem,
    halo_send,
    cross_sem,
    cross_send,
    relay_send,
    row_send,
    row_sem,
    lower_ready,
    upper_ready,
):
    me = lax.axis_index("seq")
    z = me // cols
    i = lax.rem(me, cols)
    x = i // 2
    core = lax.rem(i, 2)
    own = PRIOR
    here = win.shape[1] - PRIOR
    group = win.shape[3] // (cols // 2)
    part = BLOCK // cols

    def device(row, place):
        return {"seq": row * cols + place}

    def send(src, dst, ssem, rsem, target):
        return pltpu.make_async_remote_copy(
            src_ref=src, dst_ref=dst, send_sem=ssem, recv_sem=rsem, device_id=target, device_id_type=MESH
        )

    loads = [
        pltpu.make_async_copy(k_ref, win.at[0, pl.ds(own, here)], load_sem.at[0]),
        pltpu.make_async_copy(v_ref, win.at[1, pl.ds(own, here)], load_sem.at[1]),
    ]
    later = [
        pltpu.make_async_copy(src, dst, load_sem.at[2 + n])
        for n, (src, dst) in enumerate(
            (
                (q_ref, q_vmem),
                (counts_ref, counts),
                (tails_ref, tails),
                (order_ref, order),
                (slots_ref, slots),
            )
        )
    ]

    barrier = pltpu.get_barrier_semaphore()

    def greet(row, place):
        pl.semaphore_signal(barrier, inc=1, device_id=device(row, place), device_id_type=MESH)

    def greet_row(k, carry):
        greet(z, lax.rem(i + k, cols))
        return carry

    lax.fori_loop(1, cols, greet_row, 0)
    line = lax.rem(z + rows - 1, rows)
    line_first, line_last = line == 0, line == rows - 1

    def row_at(place):
        return lax.rem(place + 1, rows)

    @pl.when(jnp.logical_not(line_first))
    def _():
        greet(row_at(line - 1), i)

    @pl.when(jnp.logical_not(line_last))
    def _():
        greet(row_at(line + 1), i)

    has_next = z < rows - 1
    senders = [place for place in range(cols) if place % 2 == 1 or place >= cols - 3]
    crosses = core == 1
    for place in senders:
        crosses = crosses | (i == place)
    crosses = crosses & has_next
    receives = (i == 0) & (z > 0)

    @pl.when(crosses)
    def _():
        greet(z + 1, 0)

    @pl.when(receives)
    def _():
        for place in senders:
            greet(z - 1, place)

    for load in loads + later:
        load.start()
    peers = cols - 1 + jnp.where(line_first, 0, 1) + jnp.where(line_last, 0, 1)
    pl.semaphore_wait(barrier, peers + jnp.where(crosses, 1, 0) + jnp.where(receives, len(senders), 0))
    for load in loads:
        load.wait()

    spans = {cols - 1: (PRIOR - 2, 2), cols - 2: (PRIOR - 4, 2), cols - 3: (0, 1)}
    def columns_of(g):
        return pl.ds(pl.multiple_of(g * group, group), group)

    def crossing(place, g):
        first, length = spans[place]
        n = place - (cols - 3)
        src = win.at[:, pl.ds(own + here - length, length), :, columns_of(g)]
        if place // 2 == g:
            return send(
                src,
                win.at[:, pl.ds(first, length), :, columns_of(g)],
                cross_send.at[n, g],
                halo_sem.at[0 if place == cols - 1 else 1],
                device(z + 1, 0),
            )
        return send(
            src, cross.at[:, pl.ds(first, length)], cross_send.at[n, g], cross_sem.at[n], device(z, 2 * g + 1)
        )

    for place in spans:

        @pl.when(has_next & (i == place))
        def _(place=place):
            for g in range(cols // 2):
                crossing(place, g).start()

    def next_odd():
        return send(
            win.at[:, pl.ds(own, here)],
            win.at[:, pl.ds(PRIOR - here, here)],
            halo_send.at[0],
            halo_sem.at[0],
            device(z, i + 1),
        )

    def next_even():
        return send(
            win.at[:, pl.ds(own, here)],
            win.at[:, pl.ds(PRIOR - 2 * here, here)],
            halo_send.at[1],
            halo_sem.at[1],
            device(z, i + 2),
        )

    def pass_last():
        return send(
            win.at[:, pl.ds(PRIOR - 1, 1)],
            win.at[:, pl.ds(0, 1)],
            halo_send.at[2],
            halo_sem.at[1],
            device(z, i + 2),
        )

    def pass_pair():
        return send(
            win.at[:, pl.ds(PRIOR - here, here)],
            win.at[:, pl.ds(PRIOR - 2 * here, here)],
            halo_send.at[3],
            halo_sem.at[1],
            device(z, i + 1),
        )

    def pass_single():
        return send(
            win.at[:, pl.ds(PRIOR - here - 1, 1)],
            win.at[:, pl.ds(0, 1)],
            halo_send.at[4],
            halo_sem.at[1],
            device(z, i + 1),
        )

    even = core == 0
    has_two_on = even & (i < cols - 2)

    @pl.when(i < cols - 1)
    def _():
        next_odd().start()

    @pl.when(has_two_on)
    def _():
        next_even().start()

    @pl.when(me == 0)
    def _():
        for n, ref in enumerate((k_ref, v_ref)):
            pltpu.make_async_copy(ref, win.at[n, pl.ds(PRIOR - here, here)], halo_sem.at[0]).start()
            pltpu.make_async_copy(ref, win.at[n, pl.ds(PRIOR - 2 * here, here)], halo_sem.at[1]).start()
            pltpu.make_async_copy(ref.at[pl.ds(0, 1)], win.at[n, pl.ds(0, 1)], halo_sem.at[1]).start()

    def head_columns(row):
        return pl.ds(pl.multiple_of(row * HEAD_DIM, HEAD_DIM), HEAD_DIM)

    def slice_of(place):
        return pl.ds(pl.multiple_of(place * part, part), part)

    mine = pl.ds(me * here, here)

    def give_own(k, carry):
        place = lax.rem(i + k, cols)
        send(
            win.at[:, pl.ds(own, here), slice_of(place), head_columns(z)],
            recv.at[:, mine],
            row_send,
            row_sem,
            device(z, place),
        ).start()
        return carry

    lax.fori_loop(1, cols, give_own, 0)
    recv[:, mine] = win[:, own : own + here, slice_of(i), head_columns(z)]

    @pl.when(jnp.logical_not(line_first))
    def _():
        pl.semaphore_wait(lower_ready, 1)

    @pl.when(jnp.logical_not(line_last))
    def _():
        pl.semaphore_signal(lower_ready, inc=1, device_id=device(row_at(line + 1), i), device_id_type=MESH)

    def tell(place, carry):
        pl.semaphore_signal(
            upper_ready.at[line], inc=1, device_id=device(row_at(place), i), device_id_type=MESH
        )
        return carry

    lax.fori_loop(0, line, tell, 0)

    def give_row(row):
        def give(k, carry):
            place = lax.rem(i + k, cols)
            send(
                win.at[:, pl.ds(own, here), slice_of(place), head_columns(row)],
                recv.at[:, mine],
                row_send,
                row_sem,
                device(row, place),
            ).start()
            return carry

        lax.fori_loop(0, cols, give, 0)

    def give_below(k, carry):
        give_row(row_at(line - k))
        return carry

    near = jnp.minimum(line, rows // 2)

    def give_near(k, carry):
        give_row(row_at(line - near + k))
        return carry

    lax.fori_loop(0, near, give_near, 0)

    def give_above(place, carry):
        pl.semaphore_wait(upper_ready.at[place], 1)
        give_row(row_at(place))
        return carry


    first = jnp.minimum(line + 1 + 4, rows)
    lax.fori_loop(line + 1, first, give_above, 0)

    def relay(place):
        first, length = spans[place]
        return send(
            cross.at[:, pl.ds(first, length)],
            win.at[:, pl.ds(first, length), :, columns_of(x)],
            relay_send.at[place - (cols - 3)],
            halo_sem.at[0 if place == cols - 1 else 1],
            device(z + 1, 0),
        )

    for place in spans:

        @pl.when(has_next & (core == 1) & (x != place // 2))
        def _(place=place):
            first, length = spans[place]
            span = cross.at[:, pl.ds(first, length)]
            pltpu.make_async_copy(span, span, cross_sem.at[place - (cols - 3)]).wait()
            relay(place).start()

    lax.fori_loop(near + 1, line + 1, give_below, 0)

    lax.fori_loop(first, rows, give_above, 0)

    for load in later:
        load.wait()
    block_tables(counts, tails, order, slots, small_rows, table_vmem)

    table_copy = pltpu.make_async_copy(table_vmem, table, table_sem)
    table_copy.start()
    table_copy.wait()

    late_half = win.at[:, pl.ds(PRIOR - here, here)]
    pltpu.make_async_copy(late_half, late_half, halo_sem.at[0]).wait()

    @pl.when(has_two_on)
    def _():
        pass_last().start()

    @pl.when(even)
    def _():
        pass_pair().start()

    early_half = win.at[:, pl.ds(0, PRIOR - here)]
    pltpu.make_async_copy(early_half, early_half, halo_sem.at[1]).wait()

    @pl.when(even)
    def _():
        pass_single().start()

    tokens = here * BLOCK
    span = MAXB * BLOCK - BLOCK + tokens
    query = lax.broadcasted_iota(jnp.int32, (tokens, BLOCK), 0)
    query_block = query // BLOCK
    token = lax.broadcasted_iota(jnp.int32, (tokens, BLOCK), 1)
    first_block = me * here
    query_doc = jnp.zeros((tokens, BLOCK), jnp.int32)
    query_valid = jnp.zeros((tokens, BLOCK), jnp.int32)
    for b in range(here):
        query_doc = jnp.where(query_block == b, table[0, first_block + b], query_doc)
        query_valid = jnp.where(query_block == b, table[1, first_block + b], query_valid)
    query_ok = lax.rem(query, BLOCK) < query_valid
    for b in range(PRIOR + here):
        block = first_block + b - PRIOR
        there = jnp.maximum(block, 0)
        doc = jnp.where(block >= 0, table[0, there], -1)
        limit = jnp.where(block >= 0, table[1, there], 0)
        seen = (query_doc == doc) & (token < limit) & (token + (b - PRIOR) * BLOCK <= query)
        allowed[:, b * BLOCK : (b + 1) * BLOCK] = seen.astype(F32)

    def attend(head):
        at = head_columns(head)
        keys = win[0, :, :, at].reshape(span, HEAD_DIM)
        values = win[1, :, :, at].reshape(span, HEAD_DIM)
        scores = lax.dot_general(
            q_vmem[:, at], keys, (((1,), (1,)), ((), ())), preferred_element_type=F32
        ) * (HEAD_DIM**-0.5)
        scores = jnp.where(allowed[...] > 0.5, scores, MASKED_SCORE)
        peak = jnp.max(scores, axis=1, keepdims=True)
        weights = jnp.exp(scores - peak)
        totals = jnp.sum(weights, axis=1, keepdims=True)
        mixed = jnp.dot(weights.astype(BF16), values, preferred_element_type=F32)
        att_ref[:, at] = jnp.where(query_ok, mixed / totals, 0.0).astype(BF16)

    def attend_head(head, carry):
        attend(head)
        return carry

    lax.fori_loop(0, HEADS, attend_head, 0)

    landed = recv.at[:, pl.ds(0, (rows * cols - 1) * here)]
    pltpu.make_async_copy(landed, landed, row_sem).wait()

    def place_block(c, carry):
        s = jnp.clip(table[2, c], 0, out_k.shape[0] - 1)
        out_k[c] = recv[0, s]
        out_v[c] = recv[1, s]
        return carry

    lax.fori_loop(0, out_k.shape[0], place_block, 0, unroll=8)

    pltpu.make_async_copy(landed, landed, row_send).wait()
    for place in spans:

        @pl.when(has_next & (i == place))
        def _(place=place):
            for g in range(cols // 2):
                crossing(place, g).wait_send()

        @pl.when(has_next & (core == 1) & (x != place // 2))
        def _(place=place):
            relay(place).wait_send()

    @pl.when(i < cols - 1)
    def _():
        next_odd().wait_send()

    @pl.when(has_two_on)
    def _():
        next_even().wait_send()
        pass_last().wait_send()

    @pl.when(even)
    def _():
        pass_pair().wait_send()
        pass_single().wait_send()


def local(queries, keys, values, block_counts, last_tokens, pack_order, decode_slot):
    devices = lax.axis_size("seq")
    tokens, features = queries.shape
    here = tokens // BLOCK
    cols = devices // HEADS
    rows = HEADS
    blocks = devices * here
    part = BLOCK // cols
    prompts = pack_order.shape[0]
    window = PRIOR + here
    hbm = pl.BlockSpec(memory_space=pltpu.HBM)
    vmem = pl.BlockSpec(memory_space=pltpu.VMEM)
    dma = pltpu.SemaphoreType.DMA
    regular = pltpu.SemaphoreType.REGULAR
    shapes = ((tokens, features), (blocks, part, HEAD_DIM), (blocks, part, HEAD_DIM))
    attended, cache_keys, cache_values = pl.pallas_call(
        functools.partial(exchange_kernel, rows, cols),
        out_shape=[pltpu.VMEM(shape, BF16) for shape in shapes],
        in_specs=[hbm] * 7,
        out_specs=[vmem] * 3,
        scratch_shapes=[
            pltpu.VMEM((2, window, BLOCK, features), BF16),
            pltpu.VMEM((tokens, features), BF16),
            pltpu.VMEM((2, PRIOR, BLOCK, features // (cols // 2)), BF16),
            pltpu.VMEM((2, blocks, part, HEAD_DIM), BF16),
            pltpu.VMEM((tokens, window * BLOCK), F32),
            pltpu.VMEM((1, prompts // 2), jnp.int32),
            pltpu.VMEM((1, prompts), jnp.int32),
            pltpu.VMEM((1, prompts), jnp.int32),
            pltpu.VMEM((1, prompts // 2), jnp.int32),
            pltpu.VMEM((8, prompts), jnp.int32),
            pltpu.VMEM((8, blocks), jnp.int32),
            pltpu.SMEM((8, blocks), jnp.int32),
            dma((7,)),
            dma,
            dma((2,)),
            dma((5,)),
            dma((3,)),
            dma((3, cols // 2)),
            dma((3,)),
            dma,
            dma,
            regular,
            regular((rows,)),
        ],
        compiler_params=pltpu.CompilerParams(
            collective_id=0, has_side_effects=True, vmem_limit_bytes=60 * 1024 * 1024
        ),
    )(
        queries,
        keys.reshape(here, BLOCK, features),
        values.reshape(here, BLOCK, features),
        block_counts.reshape(1, -1),
        last_tokens.reshape(1, -1),
        pack_order.reshape(1, -1),
        decode_slot.reshape(1, -1),
    )
    return (attended, cache_keys[None], cache_values[None])


def solution(mesh):
    placed = (P(("groups", "seq"), None),) * 3 + (P("groups"),) * 4
    return jax.shard_map(
        local,
        mesh=mesh,
        in_specs=placed,
        out_specs=(
            P(("groups", "seq"), None),
            P(("groups", "seq"), None, None, None),
            P(("groups", "seq"), None, None, None),
        ),
        check_vma=False,
    )
```

```python
import functools

import jax
import jax.numpy as jnp
from jax import lax
from jax.experimental import pallas as pl
from jax.experimental.pallas import tpu as pltpu
from jax.sharding import PartitionSpec as P

HEADS = 16
HEAD_DIM = 128
BLOCK = 128
MAXB = 6
PRIOR = MAXB - 1
MASKED_SCORE = -1e30
MESH = pl.DeviceIdType.MESH
BF16 = jnp.bfloat16
F32 = jnp.float32


def column(row):
    n = row.shape[1]
    diagonal = lax.broadcasted_iota(jnp.int32, (n, n), 0) == lax.broadcasted_iota(jnp.int32, (n, n), 1)
    return jnp.sum(jnp.where(diagonal, row, 0), axis=1, keepdims=True)


def pick(mask, values):
    return jnp.sum(jnp.where(mask, values, 0), axis=0, keepdims=True)


def block_tables(counts_ref, tails_ref, order_ref, slots_ref, rows_ref, table_ref):
    pairs = counts_ref.shape[1]
    prompts = order_ref.shape[1]
    blocks = table_ref.shape[1]

    def iota(shape, axis):
        return lax.broadcasted_iota(jnp.int32, shape, axis)

    rows_ref[0:1, :] = jnp.zeros((1, prompts), jnp.int32)
    rows_ref[1:2, :] = jnp.ones((1, prompts), jnp.int32)
    rows_ref[2:3, :] = jnp.full((1, prompts), 1 << 20, jnp.int32)
    rows_ref[0:1, 0:pairs] = counts_ref[...]
    rows_ref[1:2, 0:pairs] = counts_ref[...]
    rows_ref[2:3, 0:pairs] = slots_ref[...]
    counts = rows_ref[0:1, :]
    sizes = rows_ref[1:2, :]
    slots = rows_ref[2:3, :]
    order = order_ref[...]
    tails = tails_ref[...]

    square = (prompts, prompts)
    picked = iota(square, 0) == order
    packed_sizes = pick(picked, column(sizes))
    packed_tails = pick(picked, column(tails))
    ends = pick(iota(square, 0) <= iota(square, 1), column(packed_sizes))
    starts = ends - packed_sizes

    wide = (prompts, blocks)
    block = iota((1, blocks), 1)
    ends_column = column(ends)
    starts_column = column(starts)
    member = (starts_column <= block) & (block < ends_column)
    position = pick(member, iota(wide, 0))
    prompt = pick(member, column(order))
    within = block - pick(member, starts_column)
    last = block + 1 == pick(member, ends_column)
    valid = jnp.where(last, pick(member, column(packed_tails)), BLOCK)

    slot_start = pick(column(slots) < slots, column(counts) + 1)
    null = prompt >= pairs
    owner = iota(wide, 0) == jnp.where(null, prompt - pairs, prompt)
    destination = pick(owner, column(slot_start)) + jnp.where(null, pick(owner, column(counts)), within)
    full = (blocks, blocks)
    source = jnp.minimum(pick(column(destination) == iota(full, 1), iota(full, 0)), blocks - 1)

    table_ref[0:1, :] = position
    table_ref[1:2, :] = valid
    table_ref[2:3, :] = source


def exchange_kernel(
    rows,
    cols,
    q_ref,
    k_ref,
    v_ref,
    counts_ref,
    tails_ref,
    order_ref,
    slots_ref,
    att_ref,
    out_k,
    out_v,
    win,
    q_vmem,
    cross,
    recv,
    allowed,
    counts,
    tails,
    order,
    slots,
    small_rows,
    table_vmem,
    table,
    load_sem,
    table_sem,
    halo_sem,
    halo_send,
    cross_sem,
    cross_send,
    relay_send,
    row_send,
    row_sem,
    lower_ready,
    upper_ready,
):
    me = lax.axis_index("seq")
    z = me // cols
    i = lax.rem(me, cols)
    x = i // 2
    core = lax.rem(i, 2)
    own = PRIOR
    here = win.shape[1] - PRIOR
    group = win.shape[3] // (cols // 2)
    part = BLOCK // cols

    def device(row, place):
        return {"seq": row * cols + place}

    def send(src, dst, ssem, rsem, target):
        return pltpu.make_async_remote_copy(
            src_ref=src, dst_ref=dst, send_sem=ssem, recv_sem=rsem, device_id=target, device_id_type=MESH
        )

    loads = [
        pltpu.make_async_copy(k_ref, win.at[0, pl.ds(own, here)], load_sem.at[0]),
        pltpu.make_async_copy(v_ref, win.at[1, pl.ds(own, here)], load_sem.at[1]),
    ]
    later = [
        pltpu.make_async_copy(src, dst, load_sem.at[2 + n])
        for n, (src, dst) in enumerate(
            (
                (q_ref, q_vmem),
                (counts_ref, counts),
                (tails_ref, tails),
                (order_ref, order),
                (slots_ref, slots),
            )
        )
    ]

    barrier = pltpu.get_barrier_semaphore()

    def greet(row, place):
        pl.semaphore_signal(barrier, inc=1, device_id=device(row, place), device_id_type=MESH)

    def greet_row(k, carry):
        greet(z, lax.rem(i + k, cols))
        return carry

    lax.fori_loop(1, cols, greet_row, 0)
    line = lax.rem(z + rows - 1, rows)
    line_first, line_last = line == 0, line == rows - 1

    def row_at(place):
        return lax.rem(place + 1, rows)

    @pl.when(jnp.logical_not(line_first))
    def _():
        greet(row_at(line - 1), i)

    @pl.when(jnp.logical_not(line_last))
    def _():
        greet(row_at(line + 1), i)

    has_next = z < rows - 1
    senders = [place for place in range(cols) if place % 2 == 1 or place >= cols - 3]
    crosses = core == 1
    for place in senders:
        crosses = crosses | (i == place)
    crosses = crosses & has_next
    receives = (i == 0) & (z > 0)

    @pl.when(crosses)
    def _():
        greet(z + 1, 0)

    @pl.when(receives)
    def _():
        for place in senders:
            greet(z - 1, place)

    for load in loads + later:
        load.start()
    peers = cols - 1 + jnp.where(line_first, 0, 1) + jnp.where(line_last, 0, 1)
    pl.semaphore_wait(barrier, peers + jnp.where(crosses, 1, 0) + jnp.where(receives, len(senders), 0))
    for load in loads:
        load.wait()

    spans = {cols - 1: (PRIOR - 2, 2), cols - 2: (PRIOR - 4, 2), cols - 3: (0, 1)}
    def columns_of(g):
        return pl.ds(pl.multiple_of(g * group, group), group)

    def crossing(place, g):
        first, length = spans[place]
        n = place - (cols - 3)
        src = win.at[:, pl.ds(own + here - length, length), :, columns_of(g)]
        if place // 2 == g:
            return send(
                src,
                win.at[:, pl.ds(first, length), :, columns_of(g)],
                cross_send.at[n, g],
                halo_sem.at[0 if place == cols - 1 else 1],
                device(z + 1, 0),
            )
        return send(
            src, cross.at[:, pl.ds(first, length)], cross_send.at[n, g], cross_sem.at[n], device(z, 2 * g + 1)
        )

    for place in spans:

        @pl.when(has_next & (i == place))
        def _(place=place):
            for g in range(cols // 2):
                crossing(place, g).start()

    def next_odd():
        return send(
            win.at[:, pl.ds(own, here)],
            win.at[:, pl.ds(PRIOR - here, here)],
            halo_send.at[0],
            halo_sem.at[0],
            device(z, i + 1),
        )

    def next_even():
        return send(
            win.at[:, pl.ds(own, here)],
            win.at[:, pl.ds(PRIOR - 2 * here, here)],
            halo_send.at[1],
            halo_sem.at[1],
            device(z, i + 2),
        )

    def pass_last():
        return send(
            win.at[:, pl.ds(PRIOR - 1, 1)],
            win.at[:, pl.ds(0, 1)],
            halo_send.at[2],
            halo_sem.at[1],
            device(z, i + 2),
        )

    def pass_pair():
        return send(
            win.at[:, pl.ds(PRIOR - here, here)],
            win.at[:, pl.ds(PRIOR - 2 * here, here)],
            halo_send.at[3],
            halo_sem.at[1],
            device(z, i + 1),
        )

    def pass_single():
        return send(
            win.at[:, pl.ds(PRIOR - here - 1, 1)],
            win.at[:, pl.ds(0, 1)],
            halo_send.at[4],
            halo_sem.at[1],
            device(z, i + 1),
        )

    even = core == 0
    has_two_on = even & (i < cols - 2)

    @pl.when(i < cols - 1)
    def _():
        next_odd().start()

    @pl.when(has_two_on)
    def _():
        next_even().start()

    @pl.when(me == 0)
    def _():
        for n, ref in enumerate((k_ref, v_ref)):
            pltpu.make_async_copy(ref, win.at[n, pl.ds(PRIOR - here, here)], halo_sem.at[0]).start()
            pltpu.make_async_copy(ref, win.at[n, pl.ds(PRIOR - 2 * here, here)], halo_sem.at[1]).start()
            pltpu.make_async_copy(ref.at[pl.ds(0, 1)], win.at[n, pl.ds(0, 1)], halo_sem.at[1]).start()

    def head_columns(row):
        return pl.ds(pl.multiple_of(row * HEAD_DIM, HEAD_DIM), HEAD_DIM)

    def slice_of(place):
        return pl.ds(pl.multiple_of(place * part, part), part)

    mine = pl.ds(me * here, here)

    def give_own(k, carry):
        place = lax.rem(i + k, cols)
        send(
            win.at[:, pl.ds(own, here), slice_of(place), head_columns(z)],
            recv.at[:, mine],
            row_send,
            row_sem,
            device(z, place),
        ).start()
        return carry

    lax.fori_loop(1, cols, give_own, 0)
    recv[:, mine] = win[:, own : own + here, slice_of(i), head_columns(z)]

    @pl.when(jnp.logical_not(line_first))
    def _():
        pl.semaphore_wait(lower_ready, 1)

    @pl.when(jnp.logical_not(line_last))
    def _():
        pl.semaphore_signal(lower_ready, inc=1, device_id=device(row_at(line + 1), i), device_id_type=MESH)

    def tell(place, carry):
        pl.semaphore_signal(
            upper_ready.at[line], inc=1, device_id=device(row_at(place), i), device_id_type=MESH
        )
        return carry

    lax.fori_loop(0, line, tell, 0)

    def give_row(row):
        def give(k, carry):
            place = lax.rem(i + k, cols)
            send(
                win.at[:, pl.ds(own, here), slice_of(place), head_columns(row)],
                recv.at[:, mine],
                row_send,
                row_sem,
                device(row, place),
            ).start()
            return carry

        lax.fori_loop(0, cols, give, 0)

    def give_below(k, carry):
        give_row(row_at(line - k))
        return carry

    near = jnp.minimum(line, rows // 2)

    def give_near(k, carry):
        give_row(row_at(line - near + k))
        return carry

    lax.fori_loop(0, near, give_near, 0)

    def relay(place):
        first, length = spans[place]
        return send(
            cross.at[:, pl.ds(first, length)],
            win.at[:, pl.ds(first, length), :, columns_of(x)],
            relay_send.at[place - (cols - 3)],
            halo_sem.at[0 if place == cols - 1 else 1],
            device(z + 1, 0),
        )

    for place in spans:

        @pl.when(has_next & (core == 1) & (x != place // 2))
        def _(place=place):
            first, length = spans[place]
            span = cross.at[:, pl.ds(first, length)]
            pltpu.make_async_copy(span, span, cross_sem.at[place - (cols - 3)]).wait()
            relay(place).start()

    lax.fori_loop(near + 1, line + 1, give_below, 0)

    def give_above(place, carry):
        pl.semaphore_wait(upper_ready.at[place], 1)
        give_row(row_at(place))
        return carry

    lax.fori_loop(line + 1, rows, give_above, 0)

    for load in later:
        load.wait()
    block_tables(counts, tails, order, slots, small_rows, table_vmem)

    table_copy = pltpu.make_async_copy(table_vmem, table, table_sem)
    table_copy.start()
    table_copy.wait()

    late_half = win.at[:, pl.ds(PRIOR - here, here)]
    pltpu.make_async_copy(late_half, late_half, halo_sem.at[0]).wait()

    @pl.when(has_two_on)
    def _():
        pass_last().start()

    @pl.when(even)
    def _():
        pass_pair().start()

    early_half = win.at[:, pl.ds(0, PRIOR - here)]
    pltpu.make_async_copy(early_half, early_half, halo_sem.at[1]).wait()

    @pl.when(even)
    def _():
        pass_single().start()

    tokens = here * BLOCK
    span = MAXB * BLOCK - BLOCK + tokens
    query = lax.broadcasted_iota(jnp.int32, (tokens, BLOCK), 0)
    query_block = query // BLOCK
    token = lax.broadcasted_iota(jnp.int32, (tokens, BLOCK), 1)
    first_block = me * here
    query_doc = jnp.zeros((tokens, BLOCK), jnp.int32)
    query_valid = jnp.zeros((tokens, BLOCK), jnp.int32)
    for b in range(here):
        query_doc = jnp.where(query_block == b, table[0, first_block + b], query_doc)
        query_valid = jnp.where(query_block == b, table[1, first_block + b], query_valid)
    query_ok = lax.rem(query, BLOCK) < query_valid
    for b in range(PRIOR + here):
        block = first_block + b - PRIOR
        there = jnp.maximum(block, 0)
        doc = jnp.where(block >= 0, table[0, there], -1)
        limit = jnp.where(block >= 0, table[1, there], 0)
        seen = (query_doc == doc) & (token < limit) & (token + (b - PRIOR) * BLOCK <= query)
        allowed[:, b * BLOCK : (b + 1) * BLOCK] = seen.astype(F32)

    def attend(head):
        at = head_columns(head)
        keys = win[0, :, :, at].reshape(span, HEAD_DIM)
        values = win[1, :, :, at].reshape(span, HEAD_DIM)
        scores = lax.dot_general(
            q_vmem[:, at], keys, (((1,), (1,)), ((), ())), preferred_element_type=F32
        ) * (HEAD_DIM**-0.5)
        scores = jnp.where(allowed[...] > 0.5, scores, MASKED_SCORE)
        peak = jnp.max(scores, axis=1, keepdims=True)
        weights = jnp.exp(scores - peak)
        totals = jnp.sum(weights, axis=1, keepdims=True)
        mixed = jnp.dot(weights.astype(BF16), values, preferred_element_type=F32)
        att_ref[:, at] = jnp.where(query_ok, mixed / totals, 0.0).astype(BF16)

    def attend_head(head, carry):
        attend(head)
        return carry

    lax.fori_loop(0, HEADS, attend_head, 0, unroll=4)

    landed = recv.at[:, pl.ds(0, (rows * cols - 1) * here)]
    pltpu.make_async_copy(landed, landed, row_sem).wait()

    def place_block(c, carry):
        s = jnp.clip(table[2, c], 0, out_k.shape[0] - 1)
        out_k[c] = recv[0, s]
        out_v[c] = recv[1, s]
        return carry

    lax.fori_loop(0, out_k.shape[0], place_block, 0, unroll=8)

    pltpu.make_async_copy(landed, landed, row_send).wait()
    for place in spans:

        @pl.when(has_next & (i == place))
        def _(place=place):
            for g in range(cols // 2):
                crossing(place, g).wait_send()

        @pl.when(has_next & (core == 1) & (x != place // 2))
        def _(place=place):
            relay(place).wait_send()

    @pl.when(i < cols - 1)
    def _():
        next_odd().wait_send()

    @pl.when(has_two_on)
    def _():
        next_even().wait_send()
        pass_last().wait_send()

    @pl.when(even)
    def _():
        pass_pair().wait_send()
        pass_single().wait_send()


def local(queries, keys, values, block_counts, last_tokens, pack_order, decode_slot):
    devices = lax.axis_size("seq")
    tokens, features = queries.shape
    here = tokens // BLOCK
    cols = devices // HEADS
    rows = HEADS
    blocks = devices * here
    part = BLOCK // cols
    prompts = pack_order.shape[0]
    window = PRIOR + here
    hbm = pl.BlockSpec(memory_space=pltpu.HBM)
    vmem = pl.BlockSpec(memory_space=pltpu.VMEM)
    dma = pltpu.SemaphoreType.DMA
    regular = pltpu.SemaphoreType.REGULAR
    shapes = ((tokens, features), (blocks, part, HEAD_DIM), (blocks, part, HEAD_DIM))
    attended, cache_keys, cache_values = pl.pallas_call(
        functools.partial(exchange_kernel, rows, cols),
        out_shape=[pltpu.VMEM(shape, BF16) for shape in shapes],
        in_specs=[hbm] * 7,
        out_specs=[vmem] * 3,
        scratch_shapes=[
            pltpu.VMEM((2, window, BLOCK, features), BF16),
            pltpu.VMEM((tokens, features), BF16),
            pltpu.VMEM((2, PRIOR, BLOCK, features // (cols // 2)), BF16),
            pltpu.VMEM((2, blocks, part, HEAD_DIM), BF16),
            pltpu.VMEM((tokens, window * BLOCK), F32),
            pltpu.VMEM((1, prompts // 2), jnp.int32),
            pltpu.VMEM((1, prompts), jnp.int32),
            pltpu.VMEM((1, prompts), jnp.int32),
            pltpu.VMEM((1, prompts // 2), jnp.int32),
            pltpu.VMEM((8, prompts), jnp.int32),
            pltpu.VMEM((8, blocks), jnp.int32),
            pltpu.SMEM((8, blocks), jnp.int32),
            dma((7,)),
            dma,
            dma((2,)),
            dma((5,)),
            dma((3,)),
            dma((3, cols // 2)),
            dma((3,)),
            dma,
            dma,
            regular,
            regular((rows,)),
        ],
        compiler_params=pltpu.CompilerParams(
            collective_id=0, has_side_effects=True, vmem_limit_bytes=60 * 1024 * 1024
        ),
    )(
        queries,
        keys.reshape(here, BLOCK, features),
        values.reshape(here, BLOCK, features),
        block_counts.reshape(1, -1),
        last_tokens.reshape(1, -1),
        pack_order.reshape(1, -1),
        decode_slot.reshape(1, -1),
    )
    return (attended, cache_keys[None], cache_values[None])


def solution(mesh):
    placed = (P(("groups", "seq"), None),) * 3 + (P("groups"),) * 4
    return jax.shard_map(
        local,
        mesh=mesh,
        in_specs=placed,
        out_specs=(
            P(("groups", "seq"), None),
            P(("groups", "seq"), None, None, None),
            P(("groups", "seq"), None, None, None),
        ),
        check_vma=False,
    )
```
